32 devices in a mesh: data: 1 (over z), outer: 4 (over y), dap: 8 (over x, core).
Axes of the slice: x: 4, y: 4, z: 1, core: 2. Of those that a mesh axis runs over, the one named last changes fastest.
The devices are a block of a 4x4x8 slice.
Arguments:
- msa_rep: bfloat16 [512, 128, 64], P('data', ('outer', 'dap'))
- msa_mask: int32 [512, 128], P('data')
- pair_rep: float32 [128, 128, 128], P(('data', 'outer', 'dap'))
- ln_gamma: bfloat16 [64], replicated
- ln_beta: bfloat16 [64], replicated
- w_left: bfloat16 [64, 32], replicated
- b_left: bfloat16 [32], replicated
- w_right: bfloat16 [64, 32], replicated
- b_right: bfloat16 [32], replicated
- w_out: bfloat16 [1024, 128], replicated
- b_out: bfloat16 [128], replicated
Outputs:
- output 1: float32 [128, 128, 128], P(('data', 'outer', 'dap'))
- output 2: bfloat16 [512, 128, 64], P(('data', 'outer', 'dap'))
All inputs are finite; a program needn't handle non-finite values.
Results may differ from the reference program's by a relative error of at most 0.00395733.
Values are sent between devices in bfloat16 or wider.
A program may use at most 768 MiB of HBM per device.

```python
import math
import jax
import jax.numpy as jnp
from jax import lax

NUM_SEQ = 512
NUM_RES = 128
MSA_DIM = 64
PAIR_DIM = 128
OPM_DIM = 32


def setup_inputs(seed: int = 0, part: int = 0) -> dict:
    part_keys = jax.random.split(jax.random.fold_in(jax.random.key(seed), part), 5)
    shared_keys = jax.random.split(jax.random.key(seed + 1), 8)
    profile = jax.random.normal(part_keys[0], (1, NUM_RES, MSA_DIM), jnp.float32)
    noise_msa = jax.random.normal(part_keys[1], (NUM_SEQ, NUM_RES, MSA_DIM), jnp.float32)
    msa_rep = (profile + 0.7 * noise_msa).astype(jnp.bfloat16)
    coverage = jax.random.randint(part_keys[2], (NUM_SEQ, 1), 35, 100)
    mask_draws = jax.random.randint(part_keys[3], (NUM_SEQ, NUM_RES), 0, 100)
    msa_mask = (mask_draws < coverage).astype(jnp.int32)
    pair_rep = jax.random.normal(part_keys[4], (NUM_RES, NUM_RES, PAIR_DIM), jnp.float32)
    ln_gamma = (1.0 + 0.3 * jax.random.normal(shared_keys[0], (MSA_DIM,), jnp.float32)).astype(jnp.bfloat16)
    ln_beta = (0.5 * jax.random.normal(shared_keys[1], (MSA_DIM,), jnp.float32)).astype(jnp.bfloat16)
    w_left = (jax.random.normal(shared_keys[2], (MSA_DIM, OPM_DIM), jnp.float32) * MSA_DIM ** -0.5).astype(jnp.bfloat16)
    b_left = (0.5 * jax.random.normal(shared_keys[3], (OPM_DIM,), jnp.float32)).astype(jnp.bfloat16)
    w_right = (jax.random.normal(shared_keys[4], (MSA_DIM, OPM_DIM), jnp.float32) * MSA_DIM ** -0.5).astype(jnp.bfloat16)
    b_right = (0.5 * jax.random.normal(shared_keys[5], (OPM_DIM,), jnp.float32)).astype(jnp.bfloat16)
    w_out = (jax.random.normal(shared_keys[6], (OPM_DIM * OPM_DIM, PAIR_DIM), jnp.float32) / OPM_DIM).astype(jnp.bfloat16)
    b_out = (0.25 * NUM_SEQ * jax.random.normal(shared_keys[7], (PAIR_DIM,), jnp.float32)).astype(jnp.bfloat16)
    return {'msa_rep': msa_rep, 'msa_mask': msa_mask, 'pair_rep': pair_rep, 'ln_gamma': ln_gamma, 'ln_beta': ln_beta, 'w_left': w_left, 'b_left': b_left, 'w_right': w_right, 'b_right': b_right, 'w_out': w_out, 'b_out': b_out}


def project_msa(msa_blk, mask_blk, ln_gamma, ln_beta, w_left, b_left, w_right, b_right):
    msa_f32 = msa_blk.astype(jnp.float32)
    mean_x = jnp.mean(msa_f32, axis=-1, keepdims=True)
    centred = msa_f32 - mean_x
    var_x = jnp.mean(centred * centred, axis=-1, keepdims=True)
    normed = (centred * lax.rsqrt(var_x + 1e-5) * ln_gamma.astype(jnp.float32) + ln_beta.astype(jnp.float32)).astype(jnp.bfloat16)
    flat_x = normed.reshape(-1, MSA_DIM)
    keep_col = mask_blk.astype(jnp.float32).reshape(-1, 1)
    left_proj = ((jnp.dot(flat_x, w_left, preferred_element_type=jnp.float32) + b_left.astype(jnp.float32)) * keep_col).astype(jnp.bfloat16)
    right_proj = ((jnp.dot(flat_x, w_right, preferred_element_type=jnp.float32) + b_right.astype(jnp.float32)) * keep_col).astype(jnp.bfloat16)
    out_shape = mask_blk.shape + (OPM_DIM,)
    return left_proj.reshape(out_shape), right_proj.reshape(out_shape)


def reference(msa_rep, msa_mask, pair_rep, ln_gamma, ln_beta, w_left, b_left, w_right, b_right, w_out, b_out):
    seq_blk = 8
    msa_blocks = msa_rep.reshape(NUM_SEQ // seq_blk, seq_blk, NUM_RES, MSA_DIM)
    mask_blocks = msa_mask.reshape(NUM_SEQ // seq_blk, seq_blk, NUM_RES)

    def proj_block(blk_args):
        return project_msa(blk_args[0], blk_args[1], ln_gamma, ln_beta, w_left, b_left, w_right, b_right)

    left_proj, right_proj = lax.map(proj_block, (msa_blocks, mask_blocks))
    left_proj = left_proj.reshape(NUM_SEQ, NUM_RES, OPM_DIM)
    right_f32 = right_proj.reshape(NUM_SEQ, NUM_RES, OPM_DIM).astype(jnp.float32)
    mask_f32 = msa_mask.astype(jnp.float32)
    row_blk = math.gcd(NUM_RES, 2 ** int(math.log2(max(1, 2 ** 24 // (NUM_RES * OPM_DIM * OPM_DIM)))))
    row_count = NUM_RES // row_blk
    left_rows = jnp.moveaxis(left_proj.reshape(NUM_SEQ, row_count, row_blk, OPM_DIM), 1, 0)
    mask_rows = jnp.moveaxis(mask_f32.reshape(NUM_SEQ, row_count, row_blk), 1, 0)
    pair_rows = pair_rep.reshape(row_count, row_blk, NUM_RES, PAIR_DIM)
    bias_out = b_out.astype(jnp.float32)

    def row_block(blk_args):
        left_blk, mask_blk, pair_blk = blk_args
        outer_blk = jnp.einsum('sic,sjd->ijcd', left_blk.astype(jnp.float32), right_f32).astype(jnp.bfloat16)
        summed = jnp.dot(outer_blk.reshape(row_blk * NUM_RES, OPM_DIM * OPM_DIM), w_out, preferred_element_type=jnp.float32).reshape(row_blk, NUM_RES, PAIR_DIM)
        pair_norm = jnp.einsum('si,sj->ij', mask_blk, mask_f32)
        return pair_blk + (summed + bias_out) / (1e-3 + pair_norm)[:, :, None]

    pair_out = lax.map(row_block, (left_rows, mask_rows, pair_rows)).reshape(NUM_RES, NUM_RES, PAIR_DIM)
    return pair_out, msa_rep
```

```python
import functools
import jax
import jax.numpy as jnp
from jax import lax
from jax.experimental import pallas as pl
from jax.experimental.pallas import tpu as pltpu
from jax.sharding import PartitionSpec as P

LN_EPS = 1e-5
NORM_EPS = 1e-3
BF = jnp.bfloat16
F32 = jnp.float32


def dot(a, b):
    return jnp.dot(a, b, preferred_element_type=F32)


def dot_nt(a, b):
    return lax.dot_general(a, b, (((1,), (1,)), ((), ())), preferred_element_type=F32)


def kernel(ny, nx, m_in, mask_ref, gamma_ref, beta_ref, wl_ref, bl_ref, wr_ref, br_ref, wo_ref, bo_ref,
           u_ref, mo_ref,
           m16, a_all, b_all, b_scr, o_scr, w_scr, w2, mt_scr, recip, rsend, rrecv,
           s1s, s1r, as_, ar, bs, br_s, ms, mr, rs, rr_s):
    o = lax.axis_index('outer')
    d = lax.axis_index('dap')
    ndap = 2 * nx
    x = d // 2
    c = lax.rem(d, 2)
    pc = 1 - c
    me = o * ndap + d
    sq = m_in.shape[1]
    md = gamma_ref.shape[1]
    res = m_in.shape[2] // md
    cw = wl_ref.shape[1]
    zd = wo_ref.shape[1]
    nj16 = ny * res
    so = sq // ndap

    def rcopy(src, dst, ss, rs_, oo, dd):
        return pltpu.make_async_remote_copy(
            src_ref=src, dst_ref=dst, send_sem=ss, recv_sem=rs_,
            device_id={'outer': oo, 'dap': dd}, device_id_type=pl.DeviceIdType.MESH)

    def sig(sem, oo, dd):
        pl.semaphore_signal(sem, inc=1, device_id={'outer': oo, 'dap': dd}, device_id_type=pl.DeviceIdType.MESH)

    yo = [lax.rem(o + t, ny) for t in range(ny)]
    xo = [lax.rem(x + t, nx) for t in range(nx)]
    far_y = sorted(range(1, ny), key=lambda t: -min(t, ny - t))
    far_x = sorted(range(1, nx), key=lambda t: -min(t, nx - t))

    bar = pltpu.get_barrier_semaphore()
    n_bar = 0
    for t in range(1, ny):
        for cc in (c, pc):
            sig(bar, yo[t], 2 * x + cc)
            n_bar += 1
    for t in range(1, ndap):
        sig(bar, o, lax.rem(d + t, ndap))
        n_bar += 1
    pl.semaphore_wait(bar, n_bar)

    st1 = []
    for t in far_y:
        cp = rcopy(m_in.at[yo[t]], m16.at[o], s1s.at[t], s1r.at[o], yo[t], d)
        cp.start()
        st1.append(cp)

    m16[o] = m_in[o]

    def column(row):
        n = row.shape[1]
        eye = lax.broadcasted_iota(jnp.int32, (n, n), 0) == lax.broadcasted_iota(jnp.int32, (n, n), 1)
        diag = jnp.where(eye, jnp.broadcast_to(row.astype(F32), (n, n)), 0.0).astype(BF)
        return dot(diag, jnp.ones((n, sq), BF))

    def flip(w):
        n = w.shape[1]
        eye = lax.broadcasted_iota(jnp.int32, (n, n), 0) == lax.broadcasted_iota(jnp.int32, (n, n), 1)
        return dot_nt(jnp.where(eye, 1.0, 0.0).astype(BF), w).astype(BF)

    g_col = column(gamma_ref[...])
    be_col = column(beta_ref[...])
    bias_col = jnp.concatenate([column(bl_ref[...]), column(br_ref[...])], axis=0)
    w_t = jnp.concatenate([flip(wl_ref[...]), flip(wr_ref[...])], axis=0)

    mt_scr[...] = mask_ref[pl.ds(pl.multiple_of(o * sq, sq), sq), :].astype(F32).T

    def project(y):
        blk = m16[y].astype(F32).T.reshape(res, md, sq)
        mean = jnp.mean(blk, axis=1, keepdims=True)
        cen = blk - mean
        var = jnp.mean(cen * cen, axis=1, keepdims=True)
        xn = (cen * lax.rsqrt(var + LN_EPS) * g_col[None] + be_col[None]).astype(BF)
        xcat = jnp.concatenate([xn[r] for r in range(res)], axis=1)
        p = dot(w_t, xcat)
        for r in range(res):
            mrow = mt_scr[pl.ds(y * (ndap * res) + d * res + r, 1), :]
            pr = (p[:, r * sq:(r + 1) * sq] + bias_col) * mrow
            a_all[c, y * res + r] = pr[:cw].astype(BF)
            b_scr[pl.ds(y * res + r, cw, stride=nj16), :] = pr[cw:]

    project(o)

    w_scr[...] = wo_ref[...].astype(F32)
    for dp in range(2):
        for q in range(cw // 8):
            rows = jnp.concatenate(
                [w_scr[pl.ds(2 * dh + dp, cw, stride=cw), :] for dh in range(4 * q, 4 * q + 4)], axis=0)
            w2[dp * zd:(dp + 1) * zd, 4 * q * cw:4 * (q + 1) * cw] = rows.T.astype(BF)

    for t in sorted(range(1, ny), key=lambda t: min(t, ny - t)):
        rcopy(m_in.at[0], m16.at[yo[t]], s1s.at[t], s1r.at[yo[t]], yo[t], d).wait_recv()
        project(yo[t])

    b_all[:, x] = b_scr[...].reshape(cw, nj16, sq).astype(BF)

    sends = []
    cp = rcopy(a_all.at[c], a_all.at[c], as_, ar, o, 2 * x + pc)
    cp.start()
    sends.append(cp)
    for t in far_x:
        cp = rcopy(b_all.at[:, x], b_all.at[:, x], bs.at[t], br_s.at[x], o, 2 * xo[t] + c)
        cp.start()
        sends.append(cp)
    for t in range(1, ndap):
        dd = lax.rem(d + t, ndap)
        cp = rcopy(m16.at[:, pl.ds(pl.multiple_of(dd * so, so), so), :], mo_ref.at[:, d], ms.at[t], mr.at[d], o, dd)
        cp.start()
        sends.append(cp)
    mo_ref[:, d] = m16[:, pl.ds(pl.multiple_of(d * so, so), so), :]

    mb = mask_ref[...].astype(F32)
    mbt = jnp.concatenate([mb[k * sq:(k + 1) * sq].T for k in range(ny)], axis=1).astype(BF)
    mb = mb.astype(BF)
    n_res = mask_ref.shape[1]
    for r in range(res):
        hot = lax.broadcasted_iota(jnp.int32, (n_res, zd), 0) == me * res + r
        mi = dot(mb, jnp.where(hot, 1.0, 0.0).astype(BF)).astype(BF)
        recip[r] = 1.0 / (NORM_EPS + dot(mbt, mi))

    rcopy(a_all.at[pc], a_all.at[pc], as_, ar, o, 2 * x + pc).wait_recv()
    for t in range(1, nx):
        rcopy(b_all.at[:, x], b_all.at[:, xo[t]], bs.at[t], br_s.at[xo[t]], o, 2 * xo[t] + c).wait_recv()

    rows_i = 2 * nj16
    a_mat = a_all[...].reshape(rows_i * cw, sq)
    for q in range(cw // 4):
        bq = b_all[4 * q:4 * q + 4].reshape(4 * nx * nj16, sq)
        oq = dot_nt(a_mat, bq).astype(BF)
        for h in range(2):
            dh = 2 * q + h
            o_scr[:, dh * cw:(dh + 1) * cw, :] = oq[:, h * zd:(h + 1) * zd].reshape(rows_i, cw, zd)

    low = lax.broadcasted_iota(jnp.int32, (zd, zd), 1) < zd // 2

    def rows_for(y, cc):
        tiles = []
        for rp in range(res // 2):
            i0 = cc * nj16 + y * res + 2 * rp
            rhs = jnp.concatenate([o_scr[i0], o_scr[i0 + 1]], axis=1)
            p = dot(w2[...], rhs)
            keep = jnp.where(low, p[:zd, :zd], p[zd:, zd:])
            move = jnp.where(low, p[:zd, zd:], p[zd:, :zd])
            tiles.append((keep + pltpu.roll(move, zd // 2, 1)).astype(BF))
        return tiles

    for t in far_y:
        for k, cc in enumerate((c, pc)):
            for rp, tile in enumerate(rows_for(yo[t], cc)):
                rsend[t, k, rp] = tile
            cp = rcopy(rsend.at[t, k], rrecv.at[o, c], rs.at[t, k], rr_s.at[o, c], yo[t], 2 * x + cc)
            cp.start()
            sends.append(cp)
    for rp, tile in enumerate(rows_for(o, pc)):
        rsend[0, 1, rp] = tile
    cp = rcopy(rsend.at[0, 1], rrecv.at[o, c], rs.at[0, 1], rr_s.at[o, c], o, 2 * x + pc)
    cp.start()
    sends.append(cp)
    for rp, tile in enumerate(rows_for(o, c)):
        rrecv[o, c, rp] = tile

    for t in range(ny):
        for k, cc in enumerate((c, pc)):
            if t == 0 and k == 0:
                continue
            rcopy(rsend.at[t, k], rrecv.at[yo[t], cc], rs.at[t, k], rr_s.at[yo[t], cc], yo[t], 2 * x + cc).wait_recv()
    bo_row = bo_ref[...].astype(F32)
    half = zd // 2
    for rp in range(res // 2):
        tt = []
        for cc in range(2):
            s = rrecv[0, cc, rp].astype(F32)
            for k in range(1, ny):
                s = s + rrecv[k, cc, rp].astype(F32)
            tt.append(s.T)
        for r2 in range(2):
            i = 2 * rp + r2
            for xx in range(nx):
                for y in range(ny):
                    at = r2 * half + xx * nj16 + y * res
                    rows = jnp.concatenate([tt[0][at:at + res], tt[1][at:at + res]], axis=0)
                    j0 = (y * nx + xx) * 2 * res
                    u_ref[i, j0:j0 + 2 * res, :] = (rows + bo_row) * recip[i, j0:j0 + 2 * res, :]

    for t in range(1, ndap):
        dd = lax.rem(d + t, ndap)
        rcopy(m16.at[:, pl.ds(0, so), :], mo_ref.at[:, dd], ms.at[t], mr.at[dd], o, dd).wait_recv()
    for cp in st1 + sends:
        cp.wait_send()


def solution(mesh):
    dap_axes = ('outer', 'dap')
    group_axes = ('data', 'outer', 'dap')
    ny = mesh.shape['outer']
    ndap = mesh.shape['dap']
    nx = ndap // 2

    def local_step(msa, mask, pair_rows, ln_gamma, ln_beta, w_left, b_left, w_right, b_right, w_out, b_out):
        n_seq, res, md = msa.shape
        n_res = mask.shape[1]
        cw = w_left.shape[1]
        zd = w_out.shape[1]
        sq = n_seq // ny
        so = sq // ndap
        nj16 = ny * res
        row = lambda v: v.reshape(1, -1)
        vm = pl.BlockSpec(memory_space=pltpu.VMEM)
        dma = pltpu.SemaphoreType.DMA
        upd, mo = pl.pallas_call(
            functools.partial(kernel, ny, nx),
            out_shape=[jax.ShapeDtypeStruct((res, n_res, zd), F32),
                       jax.ShapeDtypeStruct((ny, ndap, so, res * md), BF)],
            in_specs=[vm] * 10,
            out_specs=[vm] * 2,
            scratch_shapes=[
                pltpu.VMEM((ny, sq, res * md), BF),
                pltpu.VMEM((2, nj16, cw, sq), BF),
                pltpu.VMEM((cw, nx, nj16, sq), BF),
                pltpu.VMEM((cw * nj16, sq), F32),
                pltpu.VMEM((2 * nj16, cw * cw // 2, zd), BF),
                pltpu.VMEM((cw * cw, zd), F32),
                pltpu.VMEM((2 * zd, cw * cw // 2), BF),
                pltpu.VMEM((n_res, sq), F32),
                pltpu.VMEM((res, n_res, zd), F32),
                pltpu.VMEM((ny, 2, res // 2, zd, zd), BF),
                pltpu.VMEM((ny, 2, res // 2, zd, zd), BF),
                dma((ny,)), dma((ny,)), dma, dma, dma((nx,)), dma((nx,)),
                dma((ndap,)), dma((ndap,)), dma((ny, 2)), dma((ny, 2)),
            ],
            compiler_params=pltpu.CompilerParams(collective_id=0, has_side_effects=True,
                                                 vmem_limit_bytes=48 * 1024 * 1024),
            name='opm',
        )(msa.reshape(ny, sq, res * md), mask, row(ln_gamma), row(ln_beta), w_left, row(b_left), w_right,
          row(b_right), w_out, row(b_out))
        msa_out = jnp.transpose(mo, (2, 0, 1, 3)).reshape(so, n_res, md)
        return pair_rows + upd, msa_out

    return jax.shard_map(local_step, mesh=mesh, in_specs=(P('data', dap_axes, None), P('data', None), P(group_axes, None, None), P(), P(), P(), P(), P(), P(), P(), P()), out_specs=(P(group_axes, None, None), P(group_axes, None, None)), check_vma=False)
```
